256 devices in a mesh: clip: 32 (over y_lo, z, core), row: 8 (over x, y_hi).
Axes of the slice: x: 4, y: 4 (y_hi: 2, y_lo: 2; y = y_hi * 2 + y_lo), z: 8, core: 2. Of those that a mesh axis runs over, the one named last changes fastest.
Arguments:
- video: bfloat16 [128, 64, 320, 128], P('clip', 'row'), may hold values from -6 to 6
- spatial_one: bfloat16 [3, 3, 320, 320], replicated, may hold values from -0.109375 to 0.109375
- spatial_two: bfloat16 [3, 3, 320, 320], replicated, may hold values from -0.109375 to 0.109375
- temporal_mix: bfloat16 [3, 320, 320], replicated, may hold values from -0.1875 to 0.1875
- bias_one: float32 [320], replicated, may hold values from -3 to 3
- bias_two: float32 [320], replicated, may hold values from -3 to 3
- bias_three: float32 [320], replicated, may hold values from -3 to 3
Outputs:
- block_out: bfloat16 [128, 64, 320, 128], P('clip', 'row')
The draws below stay inside these ranges and needn't reach their ends.
All inputs are finite; a program needn't handle non-finite values.
Results may differ from the reference program's by a relative error of at most 0.011.
Values may be sent and summed in bfloat16 or wider, within the bound.
No kernel may reach another device: no remote copies, remote signals or barrier semaphores. Data moves between devices by JAX's collectives and lax.ppermute only.
A program may use at most 128 MiB of HBM per device.

```python
import jax
import jax.numpy as jnp
from jax import lax

C = 320
W = 128
FRAMES = 128
HEIGHT = 64


def steps_of(key, extent, shards, low, top_value):
    gain, own = 1.0, jax.random.fold_in(key, 6)
    for dim, shards_of in shards:
        steps = jnp.exp(jax.random.uniform(jax.random.fold_in(own, dim), (shards_of,), jnp.float32, low / len(shards), top_value / len(shards)))
        gain = gain * jnp.repeat(steps, extent[dim] // shards_of).reshape([-1 if axis == dim else 1 for axis in range(len(extent))])
    return gain


def gaussian(key, shape, deviation, reach, cuts=(), kind=jnp.bfloat16):
    level = steps_of(key, shape, cuts, -0.22, 0.18) if cuts else 1.0
    values = jax.random.normal(key, shape, jnp.float32) * deviation * level
    return jnp.minimum(jnp.maximum(values, -reach), reach).astype(kind)


def setup_inputs(seed: int = 0) -> dict:
    keys = jax.random.split(jax.random.key(seed), 8)
    video = gaussian(keys[0], (FRAMES, HEIGHT, C, W), 1.0, 6.0, ((0, 32), (1, 8)))
    spatial_one = gaussian(keys[1], (3, 3, C, C), (9 * C) ** -0.5, 0.109375)
    spatial_two = gaussian(keys[2], (3, 3, C, C), (9 * C) ** -0.5, 0.109375)
    temporal_mix = gaussian(keys[3], (3, C, C), (3 * C) ** -0.5, 0.1875)
    bias_one = gaussian(keys[4], (C,), 0.5, 3.0, (), jnp.float32)
    bias_two = gaussian(keys[5], (C,), 0.5, 3.0, (), jnp.float32)
    bias_three = gaussian(keys[6], (C,), 0.5, 3.0, (), jnp.float32)
    return dict(video=video, spatial_one=spatial_one, spatial_two=spatial_two, temporal_mix=temporal_mix, bias_one=bias_one, bias_two=bias_two, bias_three=bias_three)


def silu_round(values):
    return jax.nn.silu(values.astype(jnp.float32)).astype(jnp.bfloat16)


def conv_frame(activated, kernel):
    height = activated.shape[0]
    width = activated.shape[2]
    padded = jnp.pad(activated, ((1, 1), (0, 0), (1, 1)))
    total = jnp.zeros((height, kernel.shape[2], width), jnp.float32)
    for row_tap in range(3):
        for column_tap in range(3):
            window = padded[row_tap:row_tap + height, :, column_tap:column_tap + width]
            total = total + jnp.einsum('oc,hcw->how', kernel[row_tap, column_tap].astype(jnp.float32), window.astype(jnp.float32))
    return total


def spatial_frame(frame, kernel, bias_vec):
    activated = silu_round(frame)
    return (frame.astype(jnp.float32) + bias_vec[:, None] + conv_frame(activated, kernel)).astype(jnp.bfloat16)


def reference(video, spatial_one, spatial_two, temporal_mix, bias_one, bias_two, bias_three):
    first_out = lax.map(lambda frame: spatial_frame(frame, spatial_one, bias_one), video)
    second_out = lax.map(lambda frame: spatial_frame(frame, spatial_two, bias_two), first_out)
    act_three = lax.map(silu_round, second_out)
    padded = jnp.pad(act_three, ((1, 1), (0, 0), (0, 0), (0, 0)))
    mix_weight = temporal_mix.astype(jnp.float32)

    def temporal_frame(frame_index):
        window = lax.dynamic_slice_in_dim(padded, frame_index, 3, 0)
        centre = lax.dynamic_index_in_dim(second_out, frame_index, 0, keepdims=False)
        total = jnp.einsum('koc,khcw->how', mix_weight, window.astype(jnp.float32))
        return (centre.astype(jnp.float32) + bias_three[:, None] + total).astype(jnp.bfloat16)

    return lax.map(temporal_frame, jnp.arange(video.shape[0], dtype=jnp.int32))
```

```python
import jax
import jax.numpy as jnp
from jax import lax
from jax.experimental import pallas as pl
from jax.experimental.pallas import tpu as pltpu
from jax.sharding import PartitionSpec as P


BF = jnp.bfloat16
F32 = jnp.float32
VM = pl.BlockSpec(memory_space=pltpu.VMEM)
SM = pl.BlockSpec(memory_space=pltpu.SMEM)
HBM = pl.BlockSpec(memory_space=pltpu.HBM)


def silu(v):
    return v * (0.5 + 0.5 * jnp.tanh(0.5 * v))


def params(mib):
    return pltpu.CompilerParams(vmem_limit_bytes=mib * 2**20)


def fill(S, base, v):
    C, W = v.shape
    a = silu(v).astype(BF)
    lane = lax.broadcasted_iota(jnp.int32, (C, W), 1)
    z = jnp.zeros_like(a)
    S[pl.ds(base, C), :] = jnp.where(lane == 0, z, pltpu.roll(a, 1, 1))
    S[pl.ds(base + C, C), :] = a
    S[pl.ds(base + 2 * C, C), :] = jnp.where(lane == W - 1, z, pltpu.roll(a, W - 1, 1))


def dot_pair(w_ref, S, base, step, depth):
    acc = None
    for k in range(0, depth, 256):
        n = min(256, depth - k)
        rhs = jnp.concatenate([S[pl.ds(base + k, n), :], S[pl.ds(base + step + k, n), :]], axis=1)
        p = jnp.dot(w_ref[:, k:k + n], rhs, preferred_element_type=F32)
        acc = p if acc is None else acc + p
    return acc


class Pipe:
    def __init__(self):
        self.pending = None

    def step(self, dots, post, fills=()):
        outs = dots()
        for f in fills:
            f()
        self.flush()
        self.pending = lambda: post(outs)

    def flush(self):
        if self.pending is not None:
            self.pending()
        self.pending = None


def halves(o):
    return [o[:, :o.shape[1] // 2], o[:, o.shape[1] // 2:]]


def row_side():
    return 1 - lax.axis_index("row") % 2


def odd_clip():
    return lax.axis_index("clip") % 2


def sends_kernel(v, a, b1, b2, sems):
    FR, H = v.shape[:2]
    side = row_side()
    ra, rb = side * (H - 2), (1 - side) * (H - 2)
    copies = [
        (v.at[:, pl.ds(ra, 2)], a),
        (v.at[pl.ds(0, 1), pl.ds(rb, 2)], b1.at[pl.ds(0, 1)]),
        (v.at[pl.ds(FR - 1, 1), pl.ds(rb, 2)], b1.at[pl.ds(1, 1)]),
        (v.at[pl.ds(1, FR - 2), pl.ds(rb, 2)], b2),
    ]
    copies = [pltpu.make_async_copy(x, y, sems.at[n]) for n, (x, y) in enumerate(copies)]
    for c in copies:
        c.start()
    for c in copies:
        c.wait()


def interior_kernel(v, k1, k2, kt, b1, b2, b3, fe, so, w1, w2, wt, bias, S1, S2, F1, m1, m2, mt, sems):
    FR, H, C, W = v.shape
    T = 3 * C
    pipe = Pipe()
    loads = [pltpu.make_async_copy(x, y, sems.at[n]) for n, (x, y) in enumerate(((k1, m1), (k2, m2), (kt, mt)))]
    for c in loads:
        c.start()

    def spread(n, src, dst, taps):
        loads[n].wait()
        for t in range(taps):
            dst[:, t * C:(t + 1) * C] = src[t // 3, t % 3] if taps == 9 else src[t]

    for n, b in enumerate((b1, b2, b3)):
        bias[n] = jnp.broadcast_to(b[...][None, :], (W, C)).T

    def rows_in(g, rows):
        def run():
            for q in range(2):
                for h in rows:
                    fill(S1.at[2 * g + q], h * T, v[2 * g + q, h].astype(F32))

        return run

    for g in range(FR // 2):
        last = g == FR // 2 - 1

        def post_one(p, g=g):
            def run(outs):
                for q in range(2):
                    for e, o in enumerate(halves(outs[q])):
                        h = 2 * p + e + 1
                        f = (v[2 * g + q, h].astype(F32) + bias[0] + o).astype(BF)
                        F1[2 * g + q, h - 1] = f
                        if h in (1, 2):
                            fe[2 * g + q, h - 1] = f
                        if h in (H - 3, H - 2):
                            fe[2 * g + q, h - (H - 3) + 2] = f
                        fill(S2.at[2 * g + q], (h - 1) * T, f.astype(F32))

            return run

        def post_two(p, g=g):
            def run(outs):
                for q in range(2):
                    for e, o in enumerate(halves(outs[q])):
                        h = 2 * p + e
                        so[2 * g + q, h] = (F1[2 * g + q, h + 1].astype(F32) + bias[1] + o).astype(BF)

            return run

        def dots(w, S, p, g=g):
            return lambda: [dot_pair(w, S.at[2 * g + q], 2 * p * T, T, 3 * T) for q in range(2)]

        if g == 0:
            rows_in(0, range(4))()
            spread(0, m1, w1, 9)
        n1, n2 = (H - 2) // 2, (H - 4) // 2
        for p in range(n1):
            more = [rows_in(g, (2 * p + 4, 2 * p + 5))] if 2 * p + 5 < H else []
            if g == 0 and p == 0:
                more.append(lambda: spread(1, m2, w2, 9))
            if g == 0 and p == 1:
                more.append(lambda: spread(2, mt, wt, 3))
            pipe.step(dots(w1, S1, p), post_one(p), more)
        for p in range(n2):
            more = [rows_in(g + 1, (2 * p, 2 * p + 1))] if not last and p < 2 else ()
            pipe.step(dots(w2, S2, p), post_two(p), more)
    pipe.flush()


def edge_kernel(frames, temporal):
    def kernel(v, ha, hb, fe, so, w1, w2, bias, se, *rest):
        H, C = v.shape[1], v.shape[2]
        T = 3 * C
        te, (S1, S2, X, Y) = (rest[:2], rest[2:]) if temporal else ((), rest)
        pipe = Pipe()
        row, rows = lax.axis_index("row"), lax.axis_size("row")
        sa = row_side()
        sides = [sa, 1 - sa]
        inside = [jnp.where(s == 0, row > 0, row < rows - 1) for s in sides]
        gains = [[jnp.where((s == e) & ~ok, 0.0, 1.0).astype(F32) for e in range(2)] for s, ok in zip(sides, inside)]
        N = len(frames)
        at = list(range(N))
        fs = list(frames)
        if temporal:
            odd = odd_clip()
            at = [odd, 1 - odd]
            fs = [frames[0] + a * (frames[1] - frames[0]) for a in at]

        def fills(n):
            f = fs[n]
            for q, s in enumerate(sides):
                b = 2 * n + q
                halo = ha.at[f] if q == 0 else hb.at[at[n]]
                for k in range(2):
                    X[b, 2 * s + k] = halo[k]
                    X[b, 2 - 2 * s + k] = v[f, s * (H - 2) + k]
                for k in range(4):
                    fill(S1.at[b], k * T, X[b, k].astype(F32))

        def dots(w, S, n):
            return lambda: [dot_pair(w, S.at[2 * n + q], 0, T, 3 * T) for q in range(2)]

        def post_one(n):
            def run(outs):
                for q, s in enumerate(sides):
                    b = 2 * n + q
                    for e, o in enumerate(halves(outs[q])):
                        x = (X[b, 1 + e].astype(F32) + bias[0] + o).astype(BF)
                        Y[b, 2 * s + e] = x
                        fill(S2.at[b], pl.multiple_of((2 * s + e) * T, T), x.astype(F32) * gains[q][e])

            return run

        def known(n):
            for q, s in enumerate(sides):
                b = 2 * n + q
                for k in range(2):
                    x = fe[fs[n], 2 * s + k]
                    Y[b, 2 - 2 * s + k] = x
                    fill(S2.at[b], pl.multiple_of((2 - 2 * s + k) * T, T), x.astype(F32))

        def post_two(n):
            def run(outs):
                for q in range(2):
                    for e, o in enumerate(halves(outs[q])):
                        y = (Y[2 * n + q, 1 + e].astype(F32) + bias[1] + o).astype(BF)
                        se[n, 2 * q + e] = y
                        if temporal:
                            te[n][e + q * (H - 2)] = silu(y.astype(F32)).astype(BF)

            return run

        def middle(n):
            if temporal:
                for h in range(H - 4):
                    te[n][h + 2] = silu(so[fs[n], h].astype(F32)).astype(BF)

        fills(0)
        for n in range(N):
            more = [lambda n=n: known(n)]
            if n + 1 < N:
                more.append(lambda n=n: fills(n + 1))
            pipe.step(dots(w1, S1, n), post_one(n), more)
        for n in range(N):
            pipe.step(dots(w2, S2, n), post_two(n), [lambda n=n: middle(n)])
        pipe.flush()

    return kernel


def temporal_kernel(so, sa, sb, own_far, own_near, far, near, wt, bias, out, S, stage, sems):
    FR, HI, C, _ = so.shape
    H = HI + 4
    pipe = Pipe()
    odd = odd_clip()
    slot = {0: (sa, odd), FR - 1: (sa, 1 - odd), 1: (sb, 0), 2: (sb, 1)}

    def second(f, h):
        if 2 <= h < H - 2:
            return so.at[f, h - 2]
        ref, n = slot[f]
        return ref.at[n, h if h < 2 else h - (H - 4)]

    def fills(p):
        for e in range(2):
            h = 2 * p + e
            for f in range(1, FR - 1):
                S[h, pl.ds((f + 1) * C, C), :] = silu(second(f, h)[...].astype(F32)).astype(BF)
            for ref, even_at, odd_at in (
                (far, 0, FR + 1), (own_far, 1, FR), (own_near, FR, 1), (near, FR + 1, 0)
            ):
                to = pl.multiple_of((even_at + odd * (odd_at - even_at)) * C, C)
                S[h, pl.ds(to, C), :] = ref[h]

    side = row_side()

    def copy(p, f):
        to = {0: side * (H - 2), H // 2 - 1: (1 - side) * (H - 2)}.get(p, 2 * p)
        return pltpu.make_async_copy(stage.at[f, pl.ds(2 * p, 2)], out.at[f, pl.ds(to, 2)], sems.at[p, f])

    def dots(p, fs):
        def run():
            outs = []
            for f in fs:
                acc = None
                for k in range(0, 3 * C, 256):
                    n = min(256, 3 * C - k)
                    rhs = jnp.concatenate([S[2 * p + e, pl.ds(f * C + k, n), :] for e in range(2)], axis=1)
                    d = jnp.dot(wt[:, k:k + n], rhs, preferred_element_type=F32)
                    acc = d if acc is None else acc + d
                outs.append(acc)
            return outs

        return run

    def post(p, fs):
        def run(outs):
            for f, o2 in zip(fs, outs):
                for e, o in enumerate(halves(o2)):
                    h = 2 * p + e
                    stage[f, h] = (second(f, h)[...].astype(F32) + bias[2] + o).astype(BF)
                copy(p, f).start()

        return run

    fills(0)
    n = H // 2
    for p in range(n):
        pipe.step(dots(p, (0, 1)), post(p, (0, 1)), [lambda p=p: fills(p + 1)] if p + 1 < n else ())
        pipe.step(dots(p, (2, 3)), post(p, (2, 3)))
    pipe.flush()
    for p in range(n):
        for f in range(FR):
            copy(p, f).wait()


def in_hbm(x):
    return pltpu.with_memory_space_constraint(x, pltpu.HBM)


def shape(*dims, dtype=BF):
    return jax.ShapeDtypeStruct(dims, dtype)


def body(video, spatial_one, spatial_two, temporal_mix, bias_one, bias_two, bias_three):
    FR, H, C, W = video.shape
    T = 3 * C
    rows = lax.axis_size("row")
    swap_a = [(i, i ^ 1) for i in range(rows)]
    swap_b = [p for i in range(1, rows - 1, 2) for p in ((i, i + 1), (i + 1, i))]
    groups = ((0, FR - 1), tuple(range(1, FR - 1)))
    own_a, own_b1, own_b2 = pl.pallas_call(
        sends_kernel,
        in_specs=[HBM],
        out_specs=[VM] * 3,
        out_shape=[shape(FR, 2, C, W), shape(2, 2, C, W), shape(FR - 2, 2, C, W)],
        scratch_shapes=[pltpu.SemaphoreType.DMA((4,))],
        compiler_params=params(8),
        name="sends",
    )(in_hbm(video))
    halo_a = lax.ppermute(own_a, "row", swap_a)
    halo_b1 = lax.ppermute(own_b1, "row", swap_b)
    halo_b2 = lax.ppermute(own_b2, "row", swap_b)
    halos = ((halo_a, halo_b1), (halo_a, halo_b2))
    fe, so, w1, w2, wt, bias = pl.pallas_call(
        interior_kernel,
        in_specs=[VM, HBM, HBM, HBM, VM, VM, VM],
        out_specs=[VM] * 6,
        out_shape=[shape(FR, 4, C, W), shape(FR, H - 4, C, W), shape(C, 9 * C), shape(C, 9 * C), shape(C, 3 * C),
                   shape(3, C, W, dtype=F32)],
        scratch_shapes=[
            pltpu.VMEM((FR, H * T, W), BF),
            pltpu.VMEM((FR, (H - 2) * T, W), BF),
            pltpu.VMEM((FR, H - 2, C, W), BF),
            pltpu.VMEM((3, 3, C, C), BF),
            pltpu.VMEM((3, 3, C, C), BF),
            pltpu.VMEM((3, C, C), BF),
            pltpu.SemaphoreType.DMA((3,)),
        ],
        compiler_params=params(40),
        name="interior",
    )(video, *map(in_hbm, (spatial_one, spatial_two, temporal_mix)), bias_one, bias_two, bias_three)

    def edges(n, temporal):
        g = groups[n]
        outs = [shape(len(g), 4, C, W)] + ([shape(H, C, W)] * 2 if temporal else [])
        return pl.pallas_call(
            edge_kernel(g, temporal),
            in_specs=[VM] * 8,
            out_specs=[VM] * len(outs),
            out_shape=outs,
            scratch_shapes=[pltpu.VMEM((2 * len(g), 4 * T, W), BF)] * 2 + [pltpu.VMEM((2 * len(g), 4, C, W), BF)] * 2,
            compiler_params=params(32),
        )(video, *halos[n], fe, so, w1, w2, bias)

    sa, own_far, own_near = edges(0, True)
    clips = lax.axis_size("clip")
    far = lax.ppermute(own_far, "clip", [p for i in range(1, clips - 1, 2) for p in ((i, i + 1), (i + 1, i))])
    near = lax.ppermute(own_near, "clip", [(i, i ^ 1) for i in range(clips)])
    (sb,) = edges(1, False)
    return pl.pallas_call(
        temporal_kernel,
        in_specs=[VM] * 9,
        out_specs=HBM,
        out_shape=shape(FR, H, C, W),
        scratch_shapes=[
            pltpu.VMEM((H, (FR + 2) * C, W), BF),
            pltpu.VMEM((FR, H, C, W), BF),
            pltpu.SemaphoreType.DMA((H // 2, FR)),
        ],
        compiler_params=params(32),
        name="temporal",
    )(so, sa, sb, own_far, own_near, far, near, wt, bias)


def solution(mesh):
    placed = (P("clip", "row", None, None), P(), P(), P(), P(), P(), P())
    return jax.shard_map(body, mesh=mesh, in_specs=placed, out_specs=P("clip", "row", None, None), check_vma=False)
```

```python
import jax
import jax.numpy as jnp
from jax import lax
from jax.experimental import pallas as pl
from jax.experimental.pallas import tpu as pltpu
from jax.sharding import PartitionSpec as P


BF = jnp.bfloat16
F32 = jnp.float32
VM = pl.BlockSpec(memory_space=pltpu.VMEM)
SM = pl.BlockSpec(memory_space=pltpu.SMEM)
HBM = pl.BlockSpec(memory_space=pltpu.HBM)


def silu(v):
    return v * (0.5 + 0.5 * jnp.tanh(0.5 * v))


def params(mib):
    return pltpu.CompilerParams(vmem_limit_bytes=mib * 2**20)


def fill(S, base, v):
    C, W = v.shape
    a = silu(v).astype(BF)
    lane = lax.broadcasted_iota(jnp.int32, (C, W), 1)
    z = jnp.zeros_like(a)
    S[pl.ds(base, C), :] = jnp.where(lane == 0, z, pltpu.roll(a, 1, 1))
    S[pl.ds(base + C, C), :] = a
    S[pl.ds(base + 2 * C, C), :] = jnp.where(lane == W - 1, z, pltpu.roll(a, W - 1, 1))


def dot_pair(w_ref, S, base, step, depth):
    acc = None
    for k in range(0, depth, 256):
        n = min(256, depth - k)
        rhs = jnp.concatenate([S[pl.ds(base + k, n), :], S[pl.ds(base + step + k, n), :]], axis=1)
        p = jnp.dot(w_ref[:, k:k + n], rhs, preferred_element_type=F32)
        acc = p if acc is None else acc + p
    return acc


class Pipe:
    def __init__(self):
        self.pending = None

    def step(self, dots, post, fills=()):
        outs = dots()
        for f in fills:
            f()
        self.flush()
        self.pending = lambda: post(outs)

    def flush(self):
        if self.pending is not None:
            self.pending()
        self.pending = None


def halves(o):
    return [o[:, :o.shape[1] // 2], o[:, o.shape[1] // 2:]]


def row_side():
    return 1 - lax.axis_index("row") % 2


def odd_clip():
    return lax.axis_index("clip") % 2


def sends_kernel(v, a, b1, b2, sems):
    FR, H = v.shape[:2]
    side = row_side()
    ra, rb = side * (H - 2), (1 - side) * (H - 2)
    copies = [
        (v.at[:, pl.ds(ra, 2)], a),
        (v.at[pl.ds(0, 1), pl.ds(rb, 2)], b1.at[pl.ds(0, 1)]),
        (v.at[pl.ds(FR - 1, 1), pl.ds(rb, 2)], b1.at[pl.ds(1, 1)]),
        (v.at[pl.ds(1, FR - 2), pl.ds(rb, 2)], b2),
    ]
    copies = [pltpu.make_async_copy(x, y, sems.at[n]) for n, (x, y) in enumerate(copies)]
    for c in copies:
        c.start()
    for c in copies:
        c.wait()


def interior_kernel(v, k1, k2, kt, b1, b2, b3, fe, so, w1, w2, wt, bias, S1, S2, F1, m1, m2, mt, c1, c2, c3, sems):
    FR, H, C, W = v.shape
    T = 3 * C
    pipe = Pipe()
    loads = [pltpu.make_async_copy(x, y, sems.at[n]) for n, (x, y) in enumerate(
        ((b1, c1), (b2, c2), (b3, c3), (k1, m1), (k2, m2), (kt, mt)))]
    for c in loads:
        c.start()

    def spread(n, src, dst):
        loads[3 + n].wait()
        for t in range(9):
            dst[:, t * C:(t + 1) * C] = src[t // 3, t % 3]

    def spread_temporal():
        loads[5].wait()
        for r in range(2):
            for t in range(3):
                wt[r, :, t * C:(t + 1) * C] = mt[2 - t if r else t]

    def spread_bias():
        for n, c in enumerate((c1, c2, c3)):
            loads[n].wait()
            bias[n] = jnp.broadcast_to(c[...][None, :], (W, C)).T

    def rows_in(g, rows):
        def run():
            for q in range(2):
                for h in rows:
                    fill(S1.at[2 * g + q], h * T, v[2 * g + q, h].astype(F32))

        return run

    for g in range(FR // 2):
        last = g == FR // 2 - 1

        def post_one(p, g=g):
            def run(outs):
                for q in range(2):
                    for e, o in enumerate(halves(outs[q])):
                        h = 2 * p + e + 1
                        f = (v[2 * g + q, h].astype(F32) + bias[0] + o).astype(BF)
                        F1[2 * g + q, h - 1] = f
                        if h in (1, 2):
                            fe[2 * g + q, h - 1] = f
                        if h in (H - 3, H - 2):
                            fe[2 * g + q, h - (H - 3) + 2] = f
                        fill(S2.at[2 * g + q], (h - 1) * T, f.astype(F32))

            return run

        def post_two(p, g=g):
            def run(outs):
                for q in range(2):
                    for e, o in enumerate(halves(outs[q])):
                        h = 2 * p + e
                        so[2 * g + q, h] = (F1[2 * g + q, h + 1].astype(F32) + bias[1] + o).astype(BF)

            return run

        def dots(w, S, p, g=g):
            return lambda: [dot_pair(w, S.at[2 * g + q], 2 * p * T, T, 3 * T) for q in range(2)]

        if g == 0:
            rows_in(0, range(4))()
            spread_bias()
            spread(0, m1, w1)
        n1, n2 = (H - 2) // 2, (H - 4) // 2
        for p in range(n1):
            more = [rows_in(g, (2 * p + 4, 2 * p + 5))] if 2 * p + 5 < H else []
            if g == 0 and p == 0:
                more.append(lambda: spread(1, m2, w2))
            if g == 0 and p == 1:
                more.append(spread_temporal)
            pipe.step(dots(w1, S1, p), post_one(p), more)
        for p in range(n2):
            more = [rows_in(g + 1, (2 * p, 2 * p + 1))] if not last and p < 2 else ()
            pipe.step(dots(w2, S2, p), post_two(p), more)
    pipe.flush()


def edge_kernel(frames, temporal):
    def kernel(v, ha, hb, fe, so, w1, w2, bias, se, *rest):
        H, C = v.shape[1], v.shape[2]
        T = 3 * C
        te, (S1, S2, X, Y) = (rest[:2], rest[2:]) if temporal else ((), rest)
        pipe = Pipe()
        row, rows = lax.axis_index("row"), lax.axis_size("row")
        sa = row_side()
        sides = [sa, 1 - sa]
        inside = [jnp.where(s == 0, row > 0, row < rows - 1) for s in sides]
        gains = [[jnp.where((s == e) & ~ok, 0.0, 1.0).astype(F32) for e in range(2)] for s, ok in zip(sides, inside)]
        N = len(frames)
        at = list(range(N))
        fs = list(frames)
        if temporal:
            odd = odd_clip()
            at = [odd, 1 - odd]
            fs = [frames[0] + a * (frames[1] - frames[0]) for a in at]

        def fills(n):
            f = fs[n]
            for q, s in enumerate(sides):
                b = 2 * n + q
                halo = ha.at[f] if q == 0 else hb.at[at[n]]
                for k in range(2):
                    X[b, 2 * s + k] = halo[k]
                    X[b, 2 - 2 * s + k] = v[f, s * (H - 2) + k]
                for k in range(4):
                    fill(S1.at[b], k * T, X[b, k].astype(F32))

        def dots(w, S, n):
            return lambda: [dot_pair(w, S.at[2 * n + q], 0, T, 3 * T) for q in range(2)]

        def post_one(n):
            def run(outs):
                for q, s in enumerate(sides):
                    b = 2 * n + q
                    for e, o in enumerate(halves(outs[q])):
                        x = (X[b, 1 + e].astype(F32) + bias[0] + o).astype(BF)
                        Y[b, 2 * s + e] = x
                        fill(S2.at[b], pl.multiple_of((2 * s + e) * T, T), x.astype(F32) * gains[q][e])

            return run

        def known(n):
            for q, s in enumerate(sides):
                b = 2 * n + q
                for k in range(2):
                    x = fe[fs[n], 2 * s + k]
                    Y[b, 2 - 2 * s + k] = x
                    fill(S2.at[b], pl.multiple_of((2 - 2 * s + k) * T, T), x.astype(F32))

        def post_two(n):
            def run(outs):
                for q in range(2):
                    for e, o in enumerate(halves(outs[q])):
                        y = (Y[2 * n + q, 1 + e].astype(F32) + bias[1] + o).astype(BF)
                        se[n, 2 * q + e] = y
                        if temporal:
                            te[n][e + q * (H - 2)] = silu(y.astype(F32)).astype(BF)

            return run

        def middle(n):
            if temporal:
                for h in range(H - 4):
                    te[n][h + 2] = silu(so[fs[n], h].astype(F32)).astype(BF)

        fills(0)
        for n in range(N):
            more = [lambda n=n: known(n)]
            if n + 1 < N:
                more.append(lambda n=n: fills(n + 1))
            pipe.step(dots(w1, S1, n), post_one(n), more)
        for n in range(N):
            pipe.step(dots(w2, S2, n), post_two(n), [lambda n=n: middle(n)])
        pipe.flush()

    return kernel


def temporal_kernel(outer):
    def kernel(so, sa, sb, own_far, own_near, *rest):
        if outer:
            far, near, act, wt, bias, _, out, stage, sems = rest
        else:
            wt, bias, out, act, stage, sems = rest
        FR, HI, C, _ = so.shape
        H = HI + 4
        pipe = Pipe()
        odd = odd_clip()
        turn = [odd, 1 - odd]
        side = row_side()
        fs = [t * (FR - 1) for t in turn] if outer else [1 + t for t in turn]
        own = [own_far, own_near]

        def second(u, h):
            if 2 <= h < H - 2:
                return so[fs[u], h - 2]
            e = h if h < 2 else h - (H - 4)
            return sa[u, e] if outer else sb[turn[u], e]

        def fills(p):
            for h in (2 * p, 2 * p + 1):
                for u in range(2):
                    act[turn[u], h] = silu(second(u, h).astype(F32)).astype(BF)

        def window(u, h):
            if outer:
                return [(far, near)[u].at[h], own[u].at[h], act.at[turn[u], h]]
            return [own[u].at[h], act.at[turn[u], h], act.at[turn[1 - u], h]]

        def column(u, h, k, n):
            parts = []
            for t, ref in enumerate(window(u, h)):
                lo, hi = max(k, t * C), min(k + n, (t + 1) * C)
                if lo < hi:
                    parts.append(ref[pl.ds(lo - t * C, hi - lo), :])
            return parts[0] if len(parts) == 1 else jnp.concatenate(parts, axis=0)

        def copy(p, u):
            to = {0: side * (H - 2), H // 2 - 1: (1 - side) * (H - 2)}.get(p, 2 * p)
            return pltpu.make_async_copy(stage.at[u, pl.ds(2 * p, 2)], out.at[fs[u], pl.ds(to, 2)], sems.at[p, u])

        def dots(p):
            def run():
                outs = []
                for u in range(2):
                    acc = None
                    for k in range(0, 3 * C, 256):
                        n = min(256, 3 * C - k)
                        rhs = jnp.concatenate([column(u, 2 * p + e, k, n) for e in range(2)], axis=1)
                        d = jnp.dot(wt[turn[u], :, k:k + n], rhs, preferred_element_type=F32)
                        acc = d if acc is None else acc + d
                    outs.append(acc)
                return outs

            return run

        def post(p):
            def run(outs):
                for u, o2 in enumerate(outs):
                    for e, o in enumerate(halves(o2)):
                        h = 2 * p + e
                        stage[u, h] = (second(u, h).astype(F32) + bias[2] + o).astype(BF)
                    copy(p, u).start()

            return run

        n = H // 2
        if not outer:
            fills(0)
        for p in range(n):
            pipe.step(dots(p), post(p), [lambda p=p: fills(p + 1)] if not outer and p + 1 < n else ())
        pipe.flush()
        for p in range(n):
            for u in range(2):
                copy(p, u).wait()

    return kernel


def in_hbm(x):
    return pltpu.with_memory_space_constraint(x, pltpu.HBM)


def shape(*dims, dtype=BF):
    return jax.ShapeDtypeStruct(dims, dtype)


def body(video, spatial_one, spatial_two, temporal_mix, bias_one, bias_two, bias_three):
    FR, H, C, W = video.shape
    T = 3 * C
    rows = lax.axis_size("row")
    swap_a = [(i, i ^ 1) for i in range(rows)]
    swap_b = [p for i in range(1, rows - 1, 2) for p in ((i, i + 1), (i + 1, i))]
    groups = ((0, FR - 1), tuple(range(1, FR - 1)))
    own_a, own_b1, own_b2 = pl.pallas_call(
        sends_kernel,
        in_specs=[HBM],
        out_specs=[VM] * 3,
        out_shape=[shape(FR, 2, C, W), shape(2, 2, C, W), shape(FR - 2, 2, C, W)],
        scratch_shapes=[pltpu.SemaphoreType.DMA((4,))],
        compiler_params=params(8),
        name="sends",
    )(in_hbm(video))
    halo_a = lax.ppermute(own_a, "row", swap_a)
    halo_b1 = lax.ppermute(own_b1, "row", swap_b)
    halo_b2 = lax.ppermute(own_b2, "row", swap_b)
    halos = ((halo_a, halo_b1), (halo_a, halo_b2))
    fe, so, w1, w2, wt, bias = pl.pallas_call(
        interior_kernel,
        in_specs=[VM] + [HBM] * 6,
        out_specs=[VM] * 6,
        out_shape=[shape(FR, 4, C, W), shape(FR, H - 4, C, W), shape(C, 9 * C), shape(C, 9 * C), shape(2, C, 3 * C),
                   shape(3, C, W, dtype=F32)],
        scratch_shapes=[
            pltpu.VMEM((FR, H * T, W), BF),
            pltpu.VMEM((FR, (H - 2) * T, W), BF),
            pltpu.VMEM((FR, H - 2, C, W), BF),
            pltpu.VMEM((3, 3, C, C), BF),
            pltpu.VMEM((3, 3, C, C), BF),
            pltpu.VMEM((3, C, C), BF),
            pltpu.VMEM((C,), F32),
            pltpu.VMEM((C,), F32),
            pltpu.VMEM((C,), F32),
            pltpu.SemaphoreType.DMA((6,)),
        ],
        compiler_params=params(40),
        name="interior",
    )(video, *map(in_hbm, (spatial_one, spatial_two, temporal_mix, bias_one, bias_two, bias_three)))

    def edges(n, temporal):
        g = groups[n]
        outs = [shape(len(g), 4, C, W)] + ([shape(H, C, W)] * 2 if temporal else [])
        return pl.pallas_call(
            edge_kernel(g, temporal),
            in_specs=[VM] * 8,
            out_specs=[VM] * len(outs),
            out_shape=outs,
            scratch_shapes=[pltpu.VMEM((2 * len(g), 4 * T, W), BF)] * 2 + [pltpu.VMEM((2 * len(g), 4, C, W), BF)] * 2,
            compiler_params=params(32),
        )(video, *halos[n], fe, so, w1, w2, bias)

    sa, own_far, own_near = edges(0, True)
    clips = lax.axis_size("clip")
    near = lax.ppermute(own_near, "clip", [(i, i ^ 1) for i in range(clips)])
    far = lax.ppermute(own_far, "clip", [p for i in range(1, clips - 1, 2) for p in ((i, i + 1), (i + 1, i))])
    (sb,) = edges(1, False)

    def temporal(outer, ins, **kw):
        outs = [pltpu.HBM((FR, H, C, W), BF)] + ([] if outer else [shape(2, H, C, W)])
        return pl.pallas_call(
            temporal_kernel(outer),
            in_specs=[VM] * (len(ins) - outer) + [HBM] * outer,
            out_specs=[HBM] + [VM] * (len(outs) - 1),
            out_shape=outs,
            scratch_shapes=[pltpu.VMEM((2, H, C, W), BF), pltpu.SemaphoreType.DMA((H // 2, 2))],
            compiler_params=params(24),
            **kw,
        )(*ins)

    out, act = temporal(0, (so, sa, sb, own_far, own_near, wt, bias), name="temporal_in")
    ins = (so, sa, sb, own_far, own_near, far, near, act, wt, bias, in_hbm(out))
    return temporal(1, ins, name="temporal_out", input_output_aliases={len(ins) - 1: 0})[0]


def solution(mesh):
    placed = (P("clip", "row", None, None), P(), P(), P(), P(), P(), P())
    return jax.shard_map(body, mesh=mesh, in_specs=placed, out_specs=P("clip", "row", None, None), check_vma=False)
```
